8 devices in a mesh: pp: 4 (over z, y, x), dp: 2 (over core).
Axes of the slice: x: 2, y: 2, z: 1, core: 2. Of those that a mesh axis runs over, the one named last changes fastest.
Arguments:
- act_in: bfloat16 [6, 32, 128, 1024], P(None, 'dp')
- loss_seed: bfloat16 [6, 32, 128, 1024], P(None, 'dp')
- w_qkv: bfloat16 [4, 1024, 48, 64], P('pp', 'dp')
- w_proj: bfloat16 [4, 1024, 1024], P('pp', 'dp')
- w_up: bfloat16 [4, 1024, 4096], P('pp', 'dp')
- w_down: bfloat16 [4, 4096, 1024], P('pp', 'dp')
Outputs:
- output 1: float32 [4, 1024, 48, 64], P('pp', 'dp')
- output 2: float32 [4, 1024, 1024], P('pp', 'dp')
- output 3: float32 [4, 1024, 4096], P('pp', 'dp')
- output 4: float32 [4, 4096, 1024], P('pp', 'dp')
- output 5: bfloat16 [6, 32, 128, 1024], P(None, 'dp', 'pp')
All inputs are finite; a program needn't handle non-finite values.
Results may differ from the reference program's by a relative error of at most 0.02.
Values are sent between devices in bfloat16 or wider.
A program may use at most 1 GiB of HBM per device.

```python
import jax
import jax.numpy as jnp
from jax import lax

MICROBATCHES = 6
DP_SIZE = 2
BATCH_DEV = 16
SEQ_LEN = 128
D_MODEL = 1024
NUM_HEADS = 16
TOTAL_LAYERS = 4

HEAD_DIM = D_MODEL // NUM_HEADS
ROWS_ALL = DP_SIZE * BATCH_DEV
NORM_EPS = 1e-6


def setup_inputs(seed: int = 0) -> dict:
    key_list = jax.random.split(jax.random.key(seed), 6)
    act_shape = (MICROBATCHES, ROWS_ALL, SEQ_LEN, D_MODEL)
    seed_scale = (MICROBATCHES * ROWS_ALL * SEQ_LEN) ** -0.5
    act_in = jax.random.normal(key_list[0], act_shape, jnp.float32).astype(jnp.bfloat16)
    loss_seed = (jax.random.normal(key_list[1], act_shape, jnp.float32) * seed_scale).astype(jnp.bfloat16)
    w_qkv = (jax.random.normal(key_list[2], (TOTAL_LAYERS, D_MODEL, 3 * NUM_HEADS, HEAD_DIM), jnp.float32) * D_MODEL ** -0.5).astype(jnp.bfloat16)
    w_proj = (jax.random.normal(key_list[3], (TOTAL_LAYERS, D_MODEL, D_MODEL), jnp.float32) * D_MODEL ** -0.5).astype(jnp.bfloat16)
    w_up = (jax.random.normal(key_list[4], (TOTAL_LAYERS, D_MODEL, 4 * D_MODEL), jnp.float32) * D_MODEL ** -0.5).astype(jnp.bfloat16)
    w_down = (jax.random.normal(key_list[5], (TOTAL_LAYERS, 4 * D_MODEL, D_MODEL), jnp.float32) * (4 * D_MODEL) ** -0.5).astype(jnp.bfloat16)
    return {'act_in': act_in, 'loss_seed': loss_seed, 'w_qkv': w_qkv, 'w_proj': w_proj, 'w_up': w_up, 'w_down': w_down}


def bf16_cast(values):
    return values.astype(jnp.bfloat16).astype(jnp.float32)


def rms_norm(hidden):
    return hidden * lax.rsqrt(jnp.mean(hidden * hidden, axis=-1, keepdims=True) + NORM_EPS)


def layer_apply(hidden, layer_w):
    w_qkv, w_proj, w_up, w_down = layer_w
    hid_f32 = hidden.astype(jnp.float32)
    normed = bf16_cast(rms_norm(hid_f32))
    qkv_act = bf16_cast(jnp.einsum('bsd,dnh->bsnh', normed, w_qkv))
    q_heads = qkv_act[:, :, :NUM_HEADS]
    k_heads = qkv_act[:, :, NUM_HEADS:2 * NUM_HEADS]
    v_heads = qkv_act[:, :, 2 * NUM_HEADS:]
    scores = jnp.einsum('bqnh,bknh->bnqk', q_heads, k_heads) * HEAD_DIM ** -0.5
    causal = jnp.arange(SEQ_LEN)[:, None] >= jnp.arange(SEQ_LEN)[None, :]
    prob_bf = bf16_cast(jax.nn.softmax(jnp.where(causal, scores, -1e30), axis=-1))
    attn_out = bf16_cast(jnp.einsum('bnqk,bknh->bqnh', prob_bf, v_heads))
    attn_flat = attn_out.reshape(hidden.shape)
    mid_f32 = bf16_cast(hid_f32 + jnp.einsum('bse,ed->bsd', attn_flat, w_proj))
    normed2 = bf16_cast(rms_norm(mid_f32))
    up_act = bf16_cast(jnp.einsum('bsd,df->bsf', normed2, w_up))
    gelu_out = bf16_cast(jax.nn.gelu(up_act, approximate=True))
    return (mid_f32 + jnp.einsum('bsf,fd->bsd', gelu_out, w_down)).astype(jnp.bfloat16)


def stack_apply(weight_set, hidden):
    def layer_step(hidden_now, layer_w):
        return layer_apply(hidden_now, layer_w), None
    final_out, _ = lax.scan(jax.checkpoint(layer_step), hidden, weight_set)
    return final_out


def reference(act_in, loss_seed, w_qkv, w_proj, w_up, w_down):
    weights = (w_qkv.astype(jnp.float32), w_proj.astype(jnp.float32), w_up.astype(jnp.float32), w_down.astype(jnp.float32))
    rows_in = act_in.reshape(MICROBATCHES * DP_SIZE, BATCH_DEV, SEQ_LEN, D_MODEL)
    rows_seed = loss_seed.reshape(MICROBATCHES * DP_SIZE, BATCH_DEV, SEQ_LEN, D_MODEL)

    def row_step(grad_sum, row_pair):
        hidden, cotangent = row_pair
        rows_out, pull_back = jax.vjp(lambda weight_set: stack_apply(weight_set, hidden), weights)
        row_grads = pull_back(cotangent)[0]
        return tuple(acc_part + grad_part for acc_part, grad_part in zip(grad_sum, row_grads)), rows_out

    zero_grads = tuple(jnp.zeros_like(w_full) for w_full in weights)
    grad_sum, outs_all = lax.scan(row_step, zero_grads, (rows_in, rows_seed))
    act_out = outs_all.reshape(MICROBATCHES, ROWS_ALL, SEQ_LEN, D_MODEL)
    return grad_sum[0], grad_sum[1], grad_sum[2], grad_sum[3], act_out
```

```python
import functools

import jax
import jax.numpy as jnp
from jax import lax
from jax.experimental import pallas as pl
from jax.experimental.pallas import tpu as pltpu
from jax.sharding import PartitionSpec as P

EPS = 1e-6
SEQ = 128
D = 1024
CHUNK = 256
HEAD = 64
NSEQ = CHUNK // SEQ
GROUP = 256
GELU_C = 0.7978845608028654
BF = jnp.bfloat16
F32 = jnp.float32
VMEM_LIMIT = 62 * 2 ** 20
WARM = (11, 8, 4, 1)


def dot_nn(a, b):
    return lax.dot_general(a, b, (((1,), (0,)), ((), ())), preferred_element_type=F32)


def dot_nt(a, b):
    return lax.dot_general(a, b, (((1,), (1,)), ((), ())), preferred_element_type=F32)


def dot_tn(a, b):
    return lax.dot_general(a, b, (((0,), (0,)), ((), ())), preferred_element_type=F32)


def rms(v):
    return v * lax.rsqrt(jnp.mean(v * v, axis=-1, keepdims=True) + EPS)


def rms_pull(v, g):
    scale = lax.rsqrt(jnp.mean(v * v, axis=-1, keepdims=True) + EPS)
    inner = jnp.mean(v * g, axis=-1, keepdims=True)
    return scale * g - v * (scale * scale * scale * inner)


def head_masks():
    lane = lax.broadcasted_iota(jnp.int32, (1, GROUP), 1) // HEAD
    return [jnp.where(lane == h, 1.0, 0.0) for h in range(GROUP // HEAD)]


def stack_heads(x, masks):
    return jnp.concatenate([x * m.astype(BF) for m in masks], axis=0)


def probs_of(q, k_stack, causal):
    scores = dot_nt(q, k_stack) * (HEAD ** -0.5)
    out = []
    for h in range(GROUP // HEAD):
        s = jnp.where(causal, scores[:, h * SEQ:(h + 1) * SEQ], -1e30)
        e = jnp.exp(s - jnp.max(s, axis=-1, keepdims=True))
        out.append(e * (1.0 / jnp.sum(e, axis=-1, keepdims=True)))
    return out


def causal_mask():
    return lax.broadcasted_iota(jnp.int32, (SEQ, SEQ), 0) >= lax.broadcasted_iota(jnp.int32, (SEQ, SEQ), 1)


def attn_fwd(qkv, attn):
    def one_seq(n, carry):
        sl = pl.ds(pl.multiple_of(n * SEQ, SEQ), SEQ)
        masks = head_masks()
        causal = causal_mask()
        for g in range(D // GROUP):
            q, k, v = [qkv[sl, pl.ds(part * D + g * GROUP, GROUP)] for part in range(3)]
            probs = probs_of(q, stack_heads(k, masks), causal)
            prob = jnp.concatenate([p.astype(BF) for p in probs], axis=1)
            attn[sl, pl.ds(g * GROUP, GROUP)] = dot_nn(prob, stack_heads(v, masks)).astype(BF)
        return carry
    lax.fori_loop(0, NSEQ, one_seq, 0)


def attn_bwd(qkv, ct_attn, ct_qkv):
    def one_seq(n, carry):
        sl = pl.ds(pl.multiple_of(n * SEQ, SEQ), SEQ)
        masks = head_masks()
        causal = causal_mask()
        for g in range(D // GROUP):
            lanes = [pl.ds(part * D + g * GROUP, GROUP) for part in range(3)]
            q, k, v = [qkv[sl, ln] for ln in lanes]
            cta = ct_attn[sl, lanes[0]]
            k_stack = stack_heads(k, masks)
            probs = probs_of(q, k_stack, causal)
            ct_prob = dot_nt(cta, stack_heads(v, masks)).astype(BF).astype(F32)
            ds = []
            for h, p in enumerate(probs):
                pd = p * ct_prob[:, h * SEQ:(h + 1) * SEQ]
                ds.append(((pd - p * jnp.sum(pd, axis=-1, keepdims=True)) * (HEAD ** -0.5)).astype(BF))
            ds = jnp.concatenate(ds, axis=1)
            prob = jnp.concatenate([p.astype(BF) for p in probs], axis=1)
            ct_qkv[sl, lanes[0]] = dot_nn(ds, k_stack).astype(BF)
            ck = dot_tn(ds, q)
            cv = dot_tn(prob, cta)
            ct_qkv[sl, lanes[1]] = sum(ck[h * SEQ:(h + 1) * SEQ] * masks[h] for h in range(GROUP // HEAD)).astype(BF)
            ct_qkv[sl, lanes[2]] = sum(cv[h * SEQ:(h + 1) * SEQ] * masks[h] for h in range(GROUP // HEAD)).astype(BF)
        return carry
    lax.fori_loop(0, NSEQ, one_seq, 0)


def pipeline_kernel(chunks, stages, *refs):
    acts, seeds, *w_parts = refs[:6]
    (h_st, normed_st, qkv_st, attn_st, mid_st, normed2_st, up_st, gelu_st,
     ctout_st, ctup_st, ctmid_st, ctqkv_st, act_out) = refs[6:19]
    (wqkv, wproj, wup, wdown, x, normed, qkv, attn, mid, normed2, up, gelu, acc, hout,
     ct, b_h, b_qkv, b_mid, b_up, ctup, ctmid, ctattn, ctqkv, ctin,
     w_local, w_send, w_recv, f_in, f_out, b_in, b_load, b_out,
     f_send, f_recv, g_send, g_recv, o_send, o_recv, o_local) = refs[19:]
    stage = lax.axis_index('pp')
    replica = lax.axis_index('dp')
    first, last = stage == 0, stage == stages - 1
    weights = (wqkv, wproj, wup, wdown)

    def weight_copies(n):
        rows = w_parts[n].shape[0]
        mine = weights[n].at[pl.ds(pl.multiple_of(replica * rows, rows), rows)]
        return (pltpu.make_async_copy(w_parts[n], mine, w_local.at[n]),
                pltpu.make_async_remote_copy(src_ref=w_parts[n], dst_ref=mine, send_sem=w_send.at[n], recv_sem=w_recv.at[n],
                                             device_id=(stage, 1 - replica), device_id_type=pl.DeviceIdType.MESH))

    for n in range(4):
        for copy in weight_copies(n):
            copy.start()

    def wait_weight(n, i):
        @pl.when(i == 0)
        def _():
            for copy in weight_copies(n):
                copy.wait()

    def send_h(i):
        return pltpu.make_async_remote_copy(
            src_ref=hout, dst_ref=h_st.at[i], send_sem=f_send, recv_sem=f_recv.at[i],
            device_id=(jnp.minimum(stage + 1, stages - 1), replica), device_id_type=pl.DeviceIdType.MESH)

    def send_ct(i):
        return pltpu.make_async_remote_copy(
            src_ref=ctin, dst_ref=ctout_st.at[i], send_sem=g_send, recv_sem=g_recv.at[i],
            device_id=(jnp.maximum(stage - 1, 0), replica), device_id_type=pl.DeviceIdType.MESH)

    part = SEQ // stages

    def send_out(i, s):
        return pltpu.make_async_remote_copy(
            src_ref=hout.at[:, pl.ds(s * part, part)], dst_ref=act_out.at[pl.ds(i * NSEQ, NSEQ)],
            send_sem=o_send.at[s], recv_sem=o_recv, device_id=(s, replica), device_id_type=pl.DeviceIdType.MESH)

    def keep_out(i):
        return pltpu.make_async_copy(hout.at[:, pl.ds((stages - 1) * part, part)], act_out.at[pl.ds(i * NSEQ, NSEQ)], o_local)

    f_bufs = ((normed, normed_st), (qkv, qkv_st), (attn, attn_st), (mid, mid_st), (normed2, normed2_st), (up, up_st), (gelu, gelu_st))
    b_bufs = ((ctup, ctup_st), (ctmid, ctmid_st), (ctqkv, ctqkv_st))

    def f_save(n, i):
        return pltpu.make_async_copy(f_bufs[n][0], f_bufs[n][1].at[i], f_out.at[n])

    def b_save(n, i):
        return pltpu.make_async_copy(b_bufs[n][0], b_bufs[n][1].at[i], b_out.at[n])

    def seed_save(i):
        return pltpu.make_async_copy(ct, ctout_st.at[i], b_out.at[3])

    def b_loads(i):
        return [pltpu.make_async_copy(qkv_st.at[i], b_qkv, b_load.at[0]),
                pltpu.make_async_copy(mid_st.at[i], b_mid, b_load.at[1]),
                pltpu.make_async_copy(up_st.at[i], b_up, b_load.at[2])]

    def either(cond, src_yes, src_no, dst, sem):
        @pl.when(cond)
        def _():
            pltpu.make_async_copy(src_yes, dst, sem).start()

        @pl.when(jnp.logical_not(cond))
        def _():
            pltpu.make_async_copy(src_no, dst, sem).start()

    def wait_sent_h(i):
        @pl.when(jnp.logical_not(last))
        def _():
            send_h(i).wait_send()

        @pl.when(last)
        def _():
            for s in range(stages - 1):
                send_out(i, s).wait_send()
            keep_out(i).wait()

    def wait_b_saves(i):
        for n in range(3):
            b_save(n, i).wait()

        @pl.when(last)
        def _():
            seed_save(i).wait()

    def forward(i):
        @pl.when(jnp.logical_not(first))
        def _():
            send_h(i).wait_recv()
        either(first, acts.at[i], h_st.at[i], x, f_in)
        wait_weight(0, i)
        pltpu.make_async_copy(acts.at[i], x, f_in).wait()
        hid = x[...].reshape(CHUNK, D).astype(F32)
        normed[...] = rms(hid).astype(BF)
        f_save(0, i).start()
        for n in range(3):
            ln = pl.ds(n * D, D)
            qkv[:, ln] = dot_nn(normed[...], wqkv[:, ln]).astype(BF)
        f_save(1, i).start()
        attn_fwd(qkv, attn)
        f_save(2, i).start()
        wait_weight(1, i)
        mid[...] = (x[...].reshape(CHUNK, D).astype(F32) + dot_nn(attn[...], wproj[...])).astype(BF)
        f_save(3, i).start()
        normed2[...] = rms(mid[...].astype(F32)).astype(BF)
        f_save(4, i).start()
        wait_weight(2, i)
        for n in range(4):
            ln = pl.ds(n * D, D)
            up_act = dot_nn(normed2[...], wup[:, ln]).astype(BF)
            up[:, ln] = up_act
            v = up_act.astype(F32)
            t = jnp.tanh(v * (GELU_C + (GELU_C * 0.044715) * (v * v)))
            gelu[:, ln] = (v * (0.5 + 0.5 * t)).astype(BF)
        f_save(5, i).start()
        f_save(6, i).start()
        wait_weight(3, i)
        acc[...] = mid[...].astype(F32) + dot_nn(gelu[...], wdown[...])

        @pl.when(i > 0)
        def _():
            wait_sent_h(i - 1)
        hout[...] = acc[...].astype(BF).reshape(NSEQ, SEQ, D)

        @pl.when(jnp.logical_not(last))
        def _():
            send_h(i).start()

        @pl.when(last)
        def _():
            for s in range(stages - 1):
                send_out(i, s).start()
            keep_out(i).start()

    def backward(i):
        @pl.when(i > 0)
        def _():
            wait_b_saves(i - 1)

        @pl.when(jnp.logical_not(last))
        def _():
            send_ct(i).wait_recv()
        either(last, seeds.at[i], ctout_st.at[i], ct, b_in)
        for copy in b_loads(i):
            copy.wait()
        pltpu.make_async_copy(seeds.at[i], ct, b_in).wait()

        @pl.when(last)
        def _():
            seed_save(i).start()
        for n in range(4):
            ln = pl.ds(n * D, D)
            ct_gelu = dot_nt(ct[...].reshape(CHUNK, D), wdown[ln, :]).astype(BF).astype(F32)
            v = b_up[:, ln].astype(F32)
            v2 = v * v
            t = jnp.tanh(v * (GELU_C + (GELU_C * 0.044715) * v2))
            slope = 0.5 * (1.0 + t) + (0.5 * v) * (1.0 - t * t) * (GELU_C + (GELU_C * 3 * 0.044715) * v2)
            ctup[:, ln] = (ct_gelu * slope).astype(BF)
        b_save(0, i).start()
        acc[...] = dot_nt(ctup[...], wup[...])
        ct_norm2 = acc[...].astype(BF).astype(F32)
        ctmid[...] = (ct[...].reshape(CHUNK, D).astype(F32) + rms_pull(b_mid[...].astype(F32), ct_norm2)).astype(BF)
        b_save(1, i).start()
        ctattn[...] = dot_nt(ctmid[...], wproj[...]).astype(BF)
        attn_bwd(b_qkv, ctattn, ctqkv)
        b_save(2, i).start()
        pltpu.make_async_copy(acts.at[i], b_h, b_load.at[3]).wait()

        @pl.when(jnp.logical_not(first))
        def _():
            acc[...] = dot_nt(ctqkv[...], wqkv[...])

            @pl.when(i > 0)
            def _():
                send_ct(i - 1).wait_send()
            ct_norm = acc[...].astype(BF).astype(F32)
            ct_hid = ctmid[...].astype(F32) + rms_pull(b_h[...].reshape(CHUNK, D).astype(F32), ct_norm)
            ctin[...] = ct_hid.astype(BF).reshape(NSEQ, SEQ, D)
            send_ct(i).start()

    warm = jnp.int32(WARM[stages - 1])
    for s in range(stages - 1):
        warm = jnp.where(stage == s, WARM[s], warm)

    def tick(t, carry):
        @pl.when((t >= 1) & (t <= chunks))
        def _():
            for n in range(7):
                f_save(n, t - 1).wait()
        j = t - warm
        b_ok = (j >= 0) & (j < chunks)

        @pl.when(b_ok)
        def _():
            for copy in b_loads(j):
                copy.start()
            either(first, acts.at[j], h_st.at[j], b_h, b_load.at[3])

        @pl.when(t < chunks)
        def _():
            forward(t)

        @pl.when(b_ok)
        def _():
            backward(j)
        return carry

    lax.fori_loop(0, chunks + max(WARM), tick, 0)
    wait_sent_h(chunks - 1)
    wait_b_saves(chunks - 1)

    @pl.when(jnp.logical_not(first))
    def _():
        send_ct(chunks - 1).wait_send()

    @pl.when(jnp.logical_not(last))
    def _():
        pltpu.make_async_copy(act_out, act_out, o_recv).wait()


ANY = pl.BlockSpec(memory_space=pl.ANY)


def run_pipeline(acts, seeds, w_parts, stages):
    chunks = acts.shape[0]

    def stash(width):
        return jax.ShapeDtypeStruct((chunks, CHUNK, width), BF)

    def vmem(*shape):
        return pltpu.VMEM(shape, BF)

    whole = (NSEQ, SEQ, D)
    like_acts = jax.ShapeDtypeStruct(acts.shape, BF)
    out_shape = [like_acts, stash(D), stash(3 * D), stash(D), stash(D), stash(D), stash(4 * D), stash(4 * D),
                 like_acts, stash(4 * D), stash(D), stash(3 * D),
                 jax.ShapeDtypeStruct((chunks * NSEQ, SEQ // stages, D), BF)]
    dma = pltpu.SemaphoreType.DMA
    scratch = [
        vmem(D, 3 * D), vmem(D, D), vmem(D, 4 * D), vmem(4 * D, D),
        vmem(*whole), vmem(CHUNK, D), vmem(CHUNK, 3 * D), vmem(CHUNK, D), vmem(CHUNK, D), vmem(CHUNK, D),
        vmem(CHUNK, 4 * D), vmem(CHUNK, 4 * D), pltpu.VMEM((CHUNK, D), F32), vmem(*whole),
        vmem(*whole), vmem(*whole), vmem(CHUNK, 3 * D), vmem(CHUNK, D), vmem(CHUNK, 4 * D), vmem(CHUNK, 4 * D),
        vmem(CHUNK, D), vmem(CHUNK, D), vmem(CHUNK, 3 * D), vmem(*whole),
        dma((4,)), dma((4,)), dma((4,)), dma, dma((7,)), dma, dma((4,)), dma((4,)),
        dma, dma((chunks,)), dma, dma((chunks,)), dma((stages - 1,)), dma, dma,
    ]
    return pl.pallas_call(
        functools.partial(pipeline_kernel, chunks, stages),
        in_specs=[ANY] * 6, out_specs=[ANY] * len(out_shape), out_shape=out_shape, scratch_shapes=scratch,
        compiler_params=pltpu.CompilerParams(has_side_effects=True, vmem_limit_bytes=VMEM_LIMIT),
        cost_estimate=pl.CostEstimate(flops=chunks * CHUNK * 24 * D * D * 2, bytes_accessed=10 ** 9, transcendentals=chunks * CHUNK * 12 * D),
        name='pipeline',
    )(acts, seeds, *w_parts)


def solution(mesh):
    stages = mesh.shape['pp']

    def device_step(act_in, loss_seed, w_qkv, w_proj, w_up, w_down):
        tokens = act_in.shape[0] * act_in.shape[1] * act_in.shape[2]
        acts = act_in.reshape(-1, NSEQ, SEQ, D)
        seeds = loss_seed.reshape(-1, NSEQ, SEQ, D)
        w_parts = (w_qkv[0].reshape(-1, 3 * D), w_proj[0], w_up[0], w_down[0])
        outs = run_pipeline(acts, seeds, w_parts, stages)
        act_out = outs[12].reshape(act_in.shape[0], act_in.shape[1], -1, D)
        (_, normed, _, attn, _, normed2, _, gelu, ct_out, ct_up, ct_mid, ct_qkv) = [
            a.reshape(tokens, -1) for a in outs[:12]]

        def weight_grad(lhs, rhs):
            return lax.psum_scatter(dot_tn(lhs, rhs), 'dp', scatter_dimension=0, tiled=True)

        g_down = weight_grad(gelu, ct_out)
        g_up = weight_grad(normed2, ct_up)
        g_qkv = weight_grad(normed, ct_qkv)
        g_proj = weight_grad(attn, ct_mid)
        return g_qkv.reshape(w_qkv.shape), g_proj[None], g_up[None], g_down[None], act_out

    weight_spec = P('pp', 'dp')
    act_spec = P(None, 'dp')
    return jax.shard_map(device_step, mesh=mesh, in_specs=(act_spec, act_spec, weight_spec, weight_spec, weight_spec, weight_spec), out_specs=(weight_spec, weight_spec, weight_spec, weight_spec, P(None, 'dp', 'pp')), check_vma=False)
```

```python
import functools

import jax
import jax.numpy as jnp
from jax import lax
from jax.experimental import pallas as pl
from jax.experimental.pallas import tpu as pltpu
from jax.sharding import PartitionSpec as P

EPS = 1e-6
SEQ = 128
D = 1024
CHUNK = 256
HEAD = 64
NSEQ = CHUNK // SEQ
SCALE = HEAD ** -0.5
FWD_LANES = 128
BWD_LANES = 256
GELU_C = 0.7978845608028654
BF = jnp.bfloat16
F32 = jnp.float32
VMEM_LIMIT = 62 * 2 ** 20
WARM = (11, 8, 4, 1)


def dot_nn(a, b):
    return lax.dot_general(a, b, (((1,), (0,)), ((), ())), preferred_element_type=F32)


def dot_nt(a, b):
    return lax.dot_general(a, b, (((1,), (1,)), ((), ())), preferred_element_type=F32)


def dot_tn(a, b):
    return lax.dot_general(a, b, (((0,), (0,)), ((), ())), preferred_element_type=F32)


def rms(v):
    return v * lax.rsqrt(jnp.mean(v * v, axis=-1, keepdims=True) + EPS)


def rms_pull(v, g):
    scale = lax.rsqrt(jnp.mean(v * v, axis=-1, keepdims=True) + EPS)
    inner = jnp.mean(v * g, axis=-1, keepdims=True)
    return scale * g - v * (scale * scale * scale * inner)


def stack_heads(x, gain):
    lane = lax.broadcasted_iota(jnp.int32, (1, x.shape[1]), 1) // HEAD
    return jnp.concatenate([x * jnp.where(lane == h, gain, 0.0).astype(BF) for h in range(x.shape[1] // HEAD)], axis=0)


def pick_heads(stacked):
    low = lax.broadcasted_iota(jnp.int32, (SEQ, 2 * HEAD), 1) < HEAD
    cols = []
    for p in range(stacked.shape[1] // (2 * HEAD)):
        lanes = slice(p * 2 * HEAD, (p + 1) * 2 * HEAD)
        row = 2 * p * SEQ
        cols.append(jnp.where(low, stacked[row:row + SEQ, lanes], stacked[row + SEQ:row + 2 * SEQ, lanes]))
    return cols[0] if len(cols) == 1 else jnp.concatenate(cols, axis=1)


def probs_of(k, q_stack):
    shape = (SEQ, q_stack.shape[0])
    seen = lax.broadcasted_iota(jnp.int32, shape, 0) <= lax.broadcasted_iota(jnp.int32, shape, 1) % SEQ
    s = jnp.where(seen, dot_nt(k, q_stack), -1e30)
    e = jnp.exp(s - jnp.max(s, axis=0, keepdims=True))
    return e * (1.0 / jnp.sum(e, axis=0, keepdims=True))


def attn_fwd(qkv, attn):
    def one_seq(n, carry):
        sl = pl.ds(pl.multiple_of(n * SEQ, SEQ), SEQ)
        for g in range(D // FWD_LANES):
            q, k, v = [qkv[sl, pl.ds(part * D + g * FWD_LANES, FWD_LANES)] for part in range(3)]
            prob = probs_of(k, stack_heads(q, SCALE)).astype(BF)
            attn[sl, pl.ds(g * FWD_LANES, FWD_LANES)] = pick_heads(dot_tn(prob, v)).astype(BF)
        return carry
    lax.fori_loop(0, NSEQ, one_seq, 0)


def attn_bwd(qkv, ct_attn, ct_qkv):
    def one_seq(n, carry):
        sl = pl.ds(pl.multiple_of(n * SEQ, SEQ), SEQ)
        for g in range(D // BWD_LANES):
            lanes = [pl.ds(part * D + g * BWD_LANES, BWD_LANES) for part in range(3)]
            q, k, v = [qkv[sl, ln] for ln in lanes]
            q_stack = stack_heads(q, SCALE)
            ct_stack = stack_heads(ct_attn[sl, lanes[0]], 1.0)
            p = probs_of(k, q_stack)
            ct_prob = dot_nt(v, ct_stack).astype(BF).astype(F32)
            pd = p * ct_prob
            ds = (pd - p * jnp.sum(pd, axis=0, keepdims=True)).astype(BF)
            ct_qkv[sl, lanes[2]] = dot_nn(p.astype(BF), ct_stack).astype(BF)
            ct_qkv[sl, lanes[1]] = dot_nn(ds, q_stack).astype(BF)
            ct_qkv[sl, lanes[0]] = (pick_heads(dot_tn(ds, k)) * SCALE).astype(BF)
        return carry
    lax.fori_loop(0, NSEQ, one_seq, 0)


def pipeline_kernel(chunks, stages, *refs):
    acts, seeds, *w_parts = refs[:6]
    (h_st, normed_st, qkv_st, attn_st, mid_st, normed2_st, up_st, gelu_st,
     ctout_st, ctup_st, ctmid_st, ctqkv_st, act_out) = refs[6:19]
    (wqkv, wproj, wup, wdown, x, normed, qkv, attn, mid, normed2, up, gelu, acc, hout,
     ct, b_h, b_qkv, b_mid, b_up, ctup, ctmid, ctattn, ctqkv, ctin,
     w_local, w_send, w_recv, f_in, f_out, b_in, b_load, b_out,
     f_send, f_recv, g_send, g_recv, o_send, o_recv, o_local) = refs[19:]
    stage = lax.axis_index('pp')
    replica = lax.axis_index('dp')
    first, last = stage == 0, stage == stages - 1
    weights = (wqkv, wproj, wup, wdown)

    def weight_copies(n):
        rows = w_parts[n].shape[0]
        mine = weights[n].at[pl.ds(pl.multiple_of(replica * rows, rows), rows)]
        return (pltpu.make_async_copy(w_parts[n], mine, w_local.at[n]),
                pltpu.make_async_remote_copy(src_ref=w_parts[n], dst_ref=mine, send_sem=w_send.at[n], recv_sem=w_recv.at[n],
                                             device_id=(stage, 1 - replica), device_id_type=pl.DeviceIdType.MESH))

    for n in range(4):
        for copy in weight_copies(n):
            copy.start()

    def wait_weight(n, i):
        @pl.when(i == 0)
        def _():
            for copy in weight_copies(n):
                copy.wait()

    def send_h(i):
        return pltpu.make_async_remote_copy(
            src_ref=hout, dst_ref=h_st.at[i], send_sem=f_send, recv_sem=f_recv.at[i],
            device_id=(jnp.minimum(stage + 1, stages - 1), replica), device_id_type=pl.DeviceIdType.MESH)

    def send_ct(i):
        return pltpu.make_async_remote_copy(
            src_ref=ctin, dst_ref=ctout_st.at[i], send_sem=g_send, recv_sem=g_recv.at[i],
            device_id=(jnp.maximum(stage - 1, 0), replica), device_id_type=pl.DeviceIdType.MESH)

    part = SEQ // stages

    def send_out(i, s):
        return pltpu.make_async_remote_copy(
            src_ref=hout.at[:, pl.ds(s * part, part)], dst_ref=act_out.at[pl.ds(i * NSEQ, NSEQ)],
            send_sem=o_send.at[s], recv_sem=o_recv, device_id=(s, replica), device_id_type=pl.DeviceIdType.MESH)

    def keep_out(i):
        return pltpu.make_async_copy(hout.at[:, pl.ds((stages - 1) * part, part)], act_out.at[pl.ds(i * NSEQ, NSEQ)], o_local)

    f_bufs = ((normed, normed_st), (qkv, qkv_st), (attn, attn_st), (mid, mid_st), (normed2, normed2_st), (up, up_st), (gelu, gelu_st))
    b_bufs = ((ctup, ctup_st), (ctmid, ctmid_st), (ctqkv, ctqkv_st))

    def f_save(n, i):
        return pltpu.make_async_copy(f_bufs[n][0], f_bufs[n][1].at[i], f_out.at[n])

    def b_save(n, i):
        return pltpu.make_async_copy(b_bufs[n][0], b_bufs[n][1].at[i], b_out.at[n])

    def seed_save(i):
        return pltpu.make_async_copy(ct, ctout_st.at[i], b_out.at[3])

    def b_loads(i):
        return [pltpu.make_async_copy(qkv_st.at[i], b_qkv, b_load.at[0]),
                pltpu.make_async_copy(mid_st.at[i], b_mid, b_load.at[1]),
                pltpu.make_async_copy(up_st.at[i], b_up, b_load.at[2])]

    def either(cond, src_yes, src_no, dst, sem):
        @pl.when(cond)
        def _():
            pltpu.make_async_copy(src_yes, dst, sem).start()

        @pl.when(jnp.logical_not(cond))
        def _():
            pltpu.make_async_copy(src_no, dst, sem).start()

    def wait_sent_h(i):
        @pl.when(jnp.logical_not(last))
        def _():
            send_h(i).wait_send()

        @pl.when(last)
        def _():
            for s in range(stages - 1):
                send_out(i, s).wait_send()
            keep_out(i).wait()

    def wait_b_saves(i):
        for n in range(3):
            b_save(n, i).wait()

    def fetch_x(i):
        @pl.when(jnp.logical_not(first))
        def _():
            send_h(i).wait_recv()
        either(first, acts.at[i], h_st.at[i], x, f_in)

    def fetch_ct(i):
        @pl.when(jnp.logical_not(last))
        def _():
            send_ct(i).wait_recv()

        @pl.when(last & (i > 0))
        def _():
            seed_save(i - 1).wait()
        either(last, seeds.at[i], ctout_st.at[i], ct, b_in)

    def forward(i, j, b_ok):
        wait_weight(0, i)
        pltpu.make_async_copy(acts.at[i], x, f_in).wait()
        hid = x[...].reshape(CHUNK, D).astype(F32)
        normed[...] = rms(hid).astype(BF)
        f_save(0, i).start()
        for n in range(3):
            ln = pl.ds(n * D, D)
            qkv[:, ln] = dot_nn(normed[...], wqkv[:, ln]).astype(BF)
        f_save(1, i).start()
        attn_fwd(qkv, attn)
        f_save(2, i).start()
        wait_weight(1, i)
        mid[...] = (x[...].reshape(CHUNK, D).astype(F32) + dot_nn(attn[...], wproj[...])).astype(BF)
        f_save(3, i).start()
        normed2[...] = rms(mid[...].astype(F32)).astype(BF)
        f_save(4, i).start()
        wait_weight(2, i)
        for n in range(4):
            ln = pl.ds(n * D, D)
            up_act = dot_nn(normed2[...], wup[:, ln]).astype(BF)
            up[:, ln] = up_act
            v = up_act.astype(F32)
            t = jnp.tanh(v * (GELU_C + (GELU_C * 0.044715) * (v * v)))
            gelu[:, ln] = (v * (0.5 + 0.5 * t)).astype(BF)
        f_save(5, i).start()
        f_save(6, i).start()
        wait_weight(3, i)

        @pl.when(b_ok)
        def _():
            fetch_ct(j)
        acc[...] = mid[...].astype(F32) + dot_nn(gelu[...], wdown[...])

        @pl.when(i > 0)
        def _():
            wait_sent_h(i - 1)
        hout[...] = acc[...].astype(BF).reshape(NSEQ, SEQ, D)

        @pl.when(jnp.logical_not(last))
        def _():
            send_h(i).start()

        @pl.when(last)
        def _():
            for s in range(stages - 1):
                send_out(i, s).start()
            keep_out(i).start()

        @pl.when(i + 1 < chunks)
        def _():
            fetch_x(i + 1)

    def backward(i):
        @pl.when(i > 0)
        def _():
            wait_b_saves(i - 1)

        for copy in b_loads(i):
            copy.wait()
        pltpu.make_async_copy(seeds.at[i], ct, b_in).wait()

        @pl.when(last)
        def _():
            seed_save(i).start()
        for n in range(4):
            ln = pl.ds(n * D, D)
            ct_gelu = dot_nt(ct[...].reshape(CHUNK, D), wdown[ln, :]).astype(BF).astype(F32)
            v = b_up[:, ln].astype(F32)
            v2 = v * v
            t = jnp.tanh(v * (GELU_C + (GELU_C * 0.044715) * v2))
            slope = 0.5 * (1.0 + t) + (0.5 * v) * (1.0 - t * t) * (GELU_C + (GELU_C * 3 * 0.044715) * v2)
            ctup[:, ln] = (ct_gelu * slope).astype(BF)
        b_save(0, i).start()
        acc[...] = dot_nt(ctup[...], wup[...])
        ct_norm2 = acc[...].astype(BF).astype(F32)
        ctmid[...] = (ct[...].reshape(CHUNK, D).astype(F32) + rms_pull(b_mid[...].astype(F32), ct_norm2)).astype(BF)
        b_save(1, i).start()
        ctattn[...] = dot_nt(ctmid[...], wproj[...]).astype(BF)
        attn_bwd(b_qkv, ctattn, ctqkv)
        b_save(2, i).start()
        pltpu.make_async_copy(acts.at[i], b_h, b_load.at[3]).wait()

        @pl.when(jnp.logical_not(first))
        def _():
            acc[...] = dot_nt(ctqkv[...], wqkv[...])

            @pl.when(i > 0)
            def _():
                send_ct(i - 1).wait_send()
            ct_norm = acc[...].astype(BF).astype(F32)
            ct_hid = ctmid[...].astype(F32) + rms_pull(b_h[...].reshape(CHUNK, D).astype(F32), ct_norm)
            ctin[...] = ct_hid.astype(BF).reshape(NSEQ, SEQ, D)
            send_ct(i).start()

    warm = jnp.int32(WARM[stages - 1])
    for s in range(stages - 1):
        warm = jnp.where(stage == s, WARM[s], warm)

    def tick(t, carry):
        @pl.when((t >= 1) & (t <= chunks))
        def _():
            for n in range(7):
                f_save(n, t - 1).wait()
        j = t - warm
        b_ok = (j >= 0) & (j < chunks)

        @pl.when(b_ok)
        def _():
            for copy in b_loads(j):
                copy.start()
            either(first, acts.at[j], h_st.at[j], b_h, b_load.at[3])

        @pl.when(t < chunks)
        def _():
            forward(t, j, b_ok)

        @pl.when(b_ok & (t >= chunks))
        def _():
            fetch_ct(j)

        @pl.when(b_ok)
        def _():
            backward(j)
        return carry

    fetch_x(0)
    lax.fori_loop(0, chunks + max(WARM), tick, 0)
    wait_sent_h(chunks - 1)
    wait_b_saves(chunks - 1)

    @pl.when(last)
    def _():
        seed_save(chunks - 1).wait()

    @pl.when(jnp.logical_not(first))
    def _():
        send_ct(chunks - 1).wait_send()

    @pl.when(jnp.logical_not(last))
    def _():
        pltpu.make_async_copy(act_out, act_out, o_recv).wait()


ANY = pl.BlockSpec(memory_space=pl.ANY)


def run_pipeline(acts, seeds, w_parts, stages):
    chunks = acts.shape[0]

    def stash(width):
        return jax.ShapeDtypeStruct((chunks, CHUNK, width), BF)

    def vmem(*shape):
        return pltpu.VMEM(shape, BF)

    whole = (NSEQ, SEQ, D)
    like_acts = jax.ShapeDtypeStruct(acts.shape, BF)
    out_shape = [like_acts, stash(D), stash(3 * D), stash(D), stash(D), stash(D), stash(4 * D), stash(4 * D),
                 like_acts, stash(4 * D), stash(D), stash(3 * D),
                 jax.ShapeDtypeStruct((chunks * NSEQ, SEQ // stages, D), BF)]
    dma = pltpu.SemaphoreType.DMA
    scratch = [
        vmem(D, 3 * D), vmem(D, D), vmem(D, 4 * D), vmem(4 * D, D),
        vmem(*whole), vmem(CHUNK, D), vmem(CHUNK, 3 * D), vmem(CHUNK, D), vmem(CHUNK, D), vmem(CHUNK, D),
        vmem(CHUNK, 4 * D), vmem(CHUNK, 4 * D), pltpu.VMEM((CHUNK, D), F32), vmem(*whole),
        vmem(*whole), vmem(*whole), vmem(CHUNK, 3 * D), vmem(CHUNK, D), vmem(CHUNK, 4 * D), vmem(CHUNK, 4 * D),
        vmem(CHUNK, D), vmem(CHUNK, D), vmem(CHUNK, 3 * D), vmem(*whole),
        dma((4,)), dma((4,)), dma((4,)), dma, dma((7,)), dma, dma((4,)), dma((4,)),
        dma, dma((chunks,)), dma, dma((chunks,)), dma((stages - 1,)), dma, dma,
    ]
    return pl.pallas_call(
        functools.partial(pipeline_kernel, chunks, stages),
        in_specs=[ANY] * 6, out_specs=[ANY] * len(out_shape), out_shape=out_shape, scratch_shapes=scratch,
        compiler_params=pltpu.CompilerParams(has_side_effects=True, vmem_limit_bytes=VMEM_LIMIT),
        cost_estimate=pl.CostEstimate(flops=chunks * CHUNK * 24 * D * D * 2, bytes_accessed=10 ** 9, transcendentals=chunks * CHUNK * 12 * D),
        name='pipeline',
    )(acts, seeds, *w_parts)


def solution(mesh):
    stages = mesh.shape['pp']

    def device_step(act_in, loss_seed, w_qkv, w_proj, w_up, w_down):
        tokens = act_in.shape[0] * act_in.shape[1] * act_in.shape[2]
        acts = act_in.reshape(-1, NSEQ, SEQ, D)
        seeds = loss_seed.reshape(-1, NSEQ, SEQ, D)
        w_parts = (w_qkv[0].reshape(-1, 3 * D), w_proj[0], w_up[0], w_down[0])
        outs = run_pipeline(acts, seeds, w_parts, stages)
        act_out = outs[12].reshape(act_in.shape[0], act_in.shape[1], -1, D)
        (_, normed, _, attn, _, normed2, _, gelu, ct_out, ct_up, ct_mid, ct_qkv) = [
            a.reshape(tokens, -1) for a in outs[:12]]

        def weight_grad(lhs, rhs):
            return lax.psum_scatter(dot_tn(lhs, rhs), 'dp', scatter_dimension=0, tiled=True)

        g_down = weight_grad(gelu, ct_out)
        g_up = weight_grad(normed2, ct_up)
        g_qkv = weight_grad(normed, ct_qkv)
        g_proj = weight_grad(attn, ct_mid)
        return g_qkv.reshape(w_qkv.shape), g_proj[None], g_up[None], g_down[None], act_out

    weight_spec = P('pp', 'dp')
    act_spec = P(None, 'dp')
    return jax.shard_map(device_step, mesh=mesh, in_specs=(act_spec, act_spec, weight_spec, weight_spec, weight_spec, weight_spec), out_specs=(weight_spec, weight_spec, weight_spec, weight_spec, P(None, 'dp', 'pp')), check_vma=False)
```
